64 devices in a mesh: data: 4 (over x, y), seq: 16 (over z, core).
Axes of the slice: x: 2, y: 2, z: 8, core: 2. Of those that a mesh axis runs over, the one named last changes fastest.
The devices are a block of a 4x4x8 slice.
Arguments:
- x: bfloat16 [32768, 4096], P(('data', 'seq')), parts along dimension 0
- g: float32 [4096], replicated
- wqkv: bfloat16 [4096, 3, 16, 256], replicated
- wo: bfloat16 [16, 256, 4096], replicated
Outputs:
- output: bfloat16 [32768, 4096], P(('data', 'seq')), parts along dimension 0
There are 4 independent parts. The reference program is written for one: setup_inputs(seed, part) draws one part's arguments, and reference() takes and returns one part's arrays. A program takes and returns all parts, laid end to end along the dimension named above; an argument that names none is the same for every part.
All inputs are finite; a program needn't handle non-finite values.
Results may differ from the reference program's by a relative error of at most 0.00311508.
Values are sent between devices in bfloat16 or wider.
A program may use at most 768 MiB of HBM per device.

```python
import jax
import jax.numpy as jnp
from jax import lax

S = 8192
D = 4096
HEADS = 16
HEAD = 256


def setup_inputs(seed: int = 0, part: int = 0) -> dict:
    k_shared, k_part = jax.random.split(jax.random.PRNGKey(seed))
    kx, kf, ku = jax.random.split(jax.random.fold_in(k_part, part), 3)
    kg, kq, ko = jax.random.split(k_shared, 3)
    r = jnp.arange(S, dtype=jnp.float32)[:, None] / S
    freq = jnp.array([0.5, 1.0, 1.5, 2.5], jnp.float32)
    phase = jax.random.uniform(kf, (4,), jnp.float32, 0.0, 2.0 * jnp.pi)
    waves = jnp.sin(2.0 * jnp.pi * r * freq + phase)
    u = jax.random.normal(ku, (4, D), jnp.float32)
    x = 0.25 * jax.random.normal(kx, (S, D), jnp.float32) + 0.35 * (waves @ u)
    g = 1.0 + 0.2 * jax.random.normal(kg, (D,), jnp.float32)
    wqkv = jax.random.normal(kq, (D, 3, HEADS, HEAD), jnp.float32) * D ** -0.5
    wo = jax.random.normal(ko, (HEADS, HEAD, D), jnp.float32) * (HEADS * HEAD) ** -0.5
    return {"x": x.astype(jnp.bfloat16), "g": g, "wqkv": wqkv.astype(jnp.bfloat16), "wo": wo.astype(jnp.bfloat16)}


def _rope(x, pos):
    half = HEAD // 2
    inv = 10000.0 ** (-jnp.arange(half, dtype=jnp.float32) * 2.0 / HEAD)
    ang = pos[:, None] * inv[None, :]
    cos = jnp.cos(ang)[:, None, :]
    sin = jnp.sin(ang)[:, None, :]
    x1, x2 = x[..., :half], x[..., half:]
    return jnp.concatenate([x1 * cos - x2 * sin, x2 * cos + x1 * sin], axis=-1)


def reference(x, g, wqkv, wo):
    xf = x.astype(jnp.float32)
    xn = (xf * lax.rsqrt(jnp.mean(xf * xf, axis=-1, keepdims=True) + 1e-5) * g).astype(jnp.bfloat16)
    qkv = jnp.dot(xn, wqkv.reshape(D, 3 * HEADS * HEAD), preferred_element_type=jnp.float32).reshape(S, 3, HEADS, HEAD)
    pos = jnp.arange(S, dtype=jnp.float32)
    q = _rope(qkv[:, 0], pos).astype(jnp.bfloat16)
    k = _rope(qkv[:, 1], pos).astype(jnp.bfloat16)
    v = qkv[:, 2].astype(jnp.bfloat16)
    qb = min(S, 512)
    nq = S // qb
    scale = HEAD ** -0.5

    def one_head(args):
        qh, kh, vh = args

        def one_block(a):
            qblk, i = a
            sc = jnp.dot(qblk, kh.T, preferred_element_type=jnp.float32) * scale
            mask = (i * qb + jnp.arange(qb))[:, None] >= jnp.arange(S)[None, :]
            sc = jnp.where(mask, sc, -jnp.inf)
            pr = jax.nn.softmax(sc, axis=-1).astype(jnp.bfloat16)
            return jnp.dot(pr, vh, preferred_element_type=jnp.float32).astype(jnp.bfloat16)

        o = lax.map(one_block, (qh.reshape(nq, qb, HEAD), jnp.arange(nq)))
        return o.reshape(S, HEAD)

    o = lax.map(one_head, (q.transpose(1, 0, 2), k.transpose(1, 0, 2), v.transpose(1, 0, 2)))
    o = o.transpose(1, 0, 2).reshape(S, HEADS * HEAD)
    y = xf + jnp.dot(o, wo.reshape(HEADS * HEAD, D), preferred_element_type=jnp.float32)
    return y.astype(jnp.bfloat16)
```

```python
import functools

import jax
import jax.numpy as jnp
from jax import lax
from jax.experimental import pallas as pl
from jax.experimental.pallas import tpu as pltpu
from jax.sharding import PartitionSpec as P

BF = jnp.bfloat16
F32 = jnp.float32
VMEM_LIMIT = 60 * 2**20


def _params(**kw):
    return pltpu.CompilerParams(vmem_limit_bytes=VMEM_LIMIT, **kw)


def _weights(w, core):
    d, n3, nh, dh = w.shape
    hc = nh // 2
    bd = 256

    def body(s, i_ref, o_ref):
        o_ref[...] = jnp.swapaxes(i_ref[:, 0], 0, 1)

    return pl.pallas_call(
        body,
        grid_spec=pltpu.PrefetchScalarGridSpec(
            num_scalar_prefetch=1,
            grid=(n3, d // bd),
            in_specs=[pl.BlockSpec((bd, 1, hc, dh), lambda c, i, s: (i, c, s[0], 0))],
            out_specs=pl.BlockSpec((hc, bd, dh), lambda c, i, s: (c, i, 0)),
        ),
        out_shape=jax.ShapeDtypeStruct((n3 * hc, d, dh), BF),
        compiler_params=_params(),
        cost_estimate=pl.CostEstimate(flops=4 * 10**10, bytes_accessed=2 * w.size, transcendentals=0),
        name="weights",
    )(core, w)


def _project(scal, widx, xs, xo, wall, cosb, sinb, cosc, sinc, tiles, outs, chunk, half, prev=None):
    r, d = xs.shape
    dh = wall.shape[-1]
    hw = dh // 2
    t_rows = cosb.shape[0]
    nt = len(tiles)
    nfull = sum(t[0] for t in tiles)
    nprev = 0 if prev is None else len(prev)
    first = {}
    last = {}
    for t, (_, _, o, _) in enumerate(tiles):
        first.setdefault(o, t)
        last[o] = t

    def body(scal_ref, widx_ref, xs_ref, xo_ref, w_ref, cosb_ref, sinb_ref, cosc_ref, sinc_ref, *rest):
        out_refs = rest[nprev:nprev + len(outs)]
        xv, acc, cs, sn, sem = rest[nprev + len(outs):]
        t = pl.program_id(0)

        @pl.when(t == 0)
        def _():
            core = scal_ref[0]
            c0 = pltpu.make_async_copy(xs_ref, xv.at[pl.ds(core * r, r)], sem.at[0])
            c1 = pltpu.make_async_copy(xo_ref, xv.at[pl.ds((1 - core) * r, r)], sem.at[1])
            c0.start()
            c1.start()
            for kk in range(2):
                b = 2 * scal_ref[1] + kk
                cc, sc = cosc_ref[pl.ds(b, 1), :], sinc_ref[pl.ds(b, 1), :]
                cb, sb = cosb_ref[...], sinb_ref[...]
                cs[kk * r:(kk + 1) * r] = cb * cc - sb * sc
                sn[kk * r:(kk + 1) * r] = sb * cc + cb * sc
            c0.wait()
            c1.wait()

        if nfull == nt:
            acc[...] = jnp.dot(xv[...], w_ref[0], preferred_element_type=F32)
        else:
            @pl.when(t < nfull)
            def _():
                acc[...] = jnp.dot(xv[...], w_ref[0], preferred_element_type=F32)

            @pl.when(t >= nfull)
            def _():
                acc[half * r:(half + 1) * r] = jnp.dot(xv[half * r:(half + 1) * r], w_ref[0], preferred_element_type=F32)

        for n, (full, kind, o, _) in enumerate(tiles):
            @pl.when(t == n)
            def _(full=full, kind=kind, o=o):
                sl = slice(0, 2 * r) if full else slice(half * r, (half + 1) * r)
                a = acc[sl, :]
                if kind == 0:
                    a = a * (dh ** -0.5)
                if kind < 2:
                    a1, a2 = a[:, :hw], a[:, hw:]
                    c, s = cs[sl, :], sn[sl, :]
                    a = jnp.concatenate([a1 * c - a2 * s, a2 * c + a1 * s], axis=-1)
                out_refs[o][...] = a.astype(BF).reshape(out_refs[o].shape)

    def omap(o):
        shape, block, index = outs[o]
        nsub = last[o] - first[o]

        def f(t, *_):
            return index(jnp.clip(t - first[o], 0, nsub))
        return pl.BlockSpec(block, f)

    any_ = pl.BlockSpec(memory_space=pl.ANY)
    const = lambda shape: pl.BlockSpec(shape, lambda t, *_: (0,) * len(shape))
    in_specs = [any_, any_, pl.BlockSpec((1, d, dh), lambda t, s, wi: (wi[t], 0, 0)),
                pl.BlockSpec((r, hw), lambda t, *_: (chunk, 0)), pl.BlockSpec((r, hw), lambda t, *_: (chunk, 0)),
                const(cosc.shape), const(sinc.shape)] + [any_] * nprev
    args = [scal, widx, xs, xo, wall, cosb, sinb, cosc, sinc] + list(prev or ())
    flops = sum(2 * (2 if t[0] else 1) * r * d * dh for t in tiles)
    return pl.pallas_call(
        body,
        grid_spec=pltpu.PrefetchScalarGridSpec(
            num_scalar_prefetch=2, grid=(nt,), in_specs=in_specs, out_specs=[omap(o) for o in range(len(outs))],
            scratch_shapes=[pltpu.VMEM((2 * r, d), BF), pltpu.VMEM((2 * r, dh), F32), pltpu.VMEM((2 * r, hw), F32),
                            pltpu.VMEM((2 * r, hw), F32), pltpu.SemaphoreType.DMA((2,))]),
        out_shape=[jax.ShapeDtypeStruct(o[0], BF) for o in outs],
        input_output_aliases={9 + i: i for i in range(nprev)},
        compiler_params=_params(),
        cost_estimate=pl.CostEstimate(flops=flops, bytes_accessed=nt * 2 * d * dh, transcendentals=0),
        name="project",
    )(*args)


def _attend(tab, head, sel, nkv, nq, f1p, f1m, f2p, f2m):
    ns, _, _, _, nj, r, dh = nkv.shape
    nchip = 2 * (ns - 1)
    qb = nj * r
    kb = 2 * qb
    sub = 2
    sb = qb // sub
    n = len(sel)
    ctr = ns // 2

    def body(tab_ref, nkv_ref, nq_ref, *rest):
        f1p_r, f1m_r, f2p_r, f2m_r = rest[:nj], rest[nj:2 * nj], rest[2 * nj:3 * nj], rest[3 * nj:4 * nj]
        o_refs = rest[4 * nj:4 * nj + n]
        ks, vs, qs, acc, ms, ls, sem = rest[4 * nj + n:]
        i = pl.program_id(0)

        @pl.when(i == 0)
        def _():
            chip = tab_ref[0]
            copies = []

            def add(src, dst):
                copies.append(pltpu.make_async_copy(src, dst, sem.at[len(copies)]))
                copies[-1].start()
            for m, e in enumerate(sel):
                add(nq_ref.at[tab_ref[1 + 3 * e], head, tab_ref[2 + 3 * e]], qs.at[m])
            for kv, buf in enumerate((ks, vs)):
                for s in range(ns):
                    b = 2 * lax.rem(chip + s - ctr + nchip, nchip)
                    add(nkv_ref.at[s, head, kv], buf.at[pl.ds(b, 2)])
                bm = 2 * lax.rem(chip - ctr - 1 + nchip, nchip)
                bp = 2 * lax.rem(chip + ctr + 1, nchip)
                bo = 2 * lax.rem(chip + ctr + 2, nchip)
                for j in range(nj):
                    add(f1p_r[j].at[kv], buf.at[pl.ds(bm, 2), j])
                    add(f1m_r[j].at[kv], buf.at[pl.ds(bp, 2), j])
                    add(f2p_r[j].at[kv], buf.at[bo, j])
                    add(f2m_r[j].at[kv], buf.at[bo + 1, j])
            for c in copies:
                c.wait()

        pb = tab_ref[3 + 3 * sel[0]]
        for m, e in enumerate(sel[1:]):
            pb = jnp.where(i == m + 1, tab_ref[3 + 3 * e], pb)
        acc[...] = jnp.zeros_like(acc)
        ms[...] = jnp.full_like(ms, -jnp.inf)
        ls[...] = jnp.zeros_like(ls)

        def step(p, masked):
            kblk = ks[pl.ds(2 * p, 2)].reshape(kb, dh)
            vblk = vs[pl.ds(2 * p, 2)].reshape(kb, dh)
            qall = qs[i].reshape(qb, dh)
            ss = [lax.dot_general(qall[a * sb:(a + 1) * sb], kblk, (((1,), (1,)), ((), ())), preferred_element_type=F32)
                  for a in range(sub)]
            for a in range(sub):
                sl = slice(a * sb, (a + 1) * sb)
                s = ss[a]
                if masked:
                    qp = pb * qb + a * sb + lax.broadcasted_iota(jnp.int32, (sb, kb), 0)
                    kp = p * kb + lax.broadcasted_iota(jnp.int32, (sb, kb), 1)
                    s = jnp.where(qp >= kp, s, -jnp.inf)
                mo = ms[sl, :]
                mn = jnp.maximum(mo, jnp.max(s, axis=1, keepdims=True))
                pr = jnp.exp(s - mn[:, :1])
                al = jnp.exp(mo - mn)
                ls[sl, :] = ls[sl, :] * al + jnp.sum(pr, axis=1, keepdims=True)
                ms[sl, :] = mn
                acc[sl, :] = acc[sl, :] * al[:, :1] + jnp.dot(pr.astype(BF), vblk, preferred_element_type=F32)

        nfull = pb // 2
        lax.fori_loop(0, nfull, lambda p, c: (step(p, False), c)[1], 0)
        step(nfull, True)
        for m in range(n):
            @pl.when(i == m)
            def _(m=m):
                o_refs[m][...] = (acc[...] / ls[:, :1]).astype(BF)

    any_ = pl.BlockSpec(memory_space=pl.ANY)
    ncopy = n + 2 * (ns + 4 * nj)
    return pl.pallas_call(
        body,
        grid_spec=pltpu.PrefetchScalarGridSpec(
            num_scalar_prefetch=1, grid=(n,), in_specs=[any_] * (2 + 4 * nj),
            out_specs=[pl.BlockSpec((qb, dh), lambda i, s: (0, 0))] * n,
            scratch_shapes=[pltpu.VMEM((2 * nchip, nj, r, dh), BF), pltpu.VMEM((2 * nchip, nj, r, dh), BF),
                            pltpu.VMEM((n, nj, r, dh), BF), pltpu.VMEM((qb, dh), F32), pltpu.VMEM((qb, 128), F32),
                            pltpu.VMEM((qb, 128), F32), pltpu.SemaphoreType.DMA((ncopy,))]),
        out_shape=[jax.ShapeDtypeStruct((qb, dh), BF)] * n,
        compiler_params=_params(),
        cost_estimate=pl.CostEstimate(flops=n * 4 * qb * dh * nchip * qb, bytes_accessed=2 * nchip * 2 * qb * dh * 2,
                                      transcendentals=n * qb * nchip * qb),
        name="attend",
    )(tab, nkv, nq, *f1p, *f1m, *f2p, *f2m)


def _out_proj(heads, pieces, wo, res, dtype):
    n = len(pieces)
    qb, dh = pieces[0].shape
    dm = wo.shape[-1]
    bn = 512

    def body(h_ref, *refs):
        o, w, res_ref, y_ref = refs[:n], refs[n:2 * n], refs[2 * n], refs[2 * n + 1]
        a = res_ref[...].astype(F32)
        for i in range(n):
            a = a + jnp.dot(o[i][...], w[i][0], preferred_element_type=F32)
        y_ref[...] = a.astype(dtype)

    return pl.pallas_call(
        body,
        grid_spec=pltpu.PrefetchScalarGridSpec(
            num_scalar_prefetch=1, grid=(dm // bn,),
            in_specs=[pl.BlockSpec((qb, dh), lambda c, h: (0, 0))] * n
            + [pl.BlockSpec((1, dh, bn), functools.partial(lambda i, c, h: (h[i], 0, c), i)) for i in range(n)]
            + [pl.BlockSpec((qb, bn), lambda c, h: (0, c))],
            out_specs=pl.BlockSpec((qb, bn), lambda c, h: (0, c))),
        out_shape=jax.ShapeDtypeStruct((qb, dm), dtype),
        compiler_params=_params(),
        cost_estimate=pl.CostEstimate(flops=2 * n * qb * dh * dm, bytes_accessed=n * dh * dm * 2 + qb * dm * 8, transcendentals=0),
        name="out_proj",
    )(heads, *pieces, *([wo] * n), res)


def solution(mesh):
    p = mesh.shape["seq"]
    rows = P(("data", "seq"), None)
    nchip = p // 2

    def dev(chip, core):
        return 2 * (chip % nchip) + core

    def perm(pairs):
        return lambda a: lax.ppermute(a, "seq", pairs)

    def chips(n):
        return perm([(dev(c, k), dev(c + n, k)) for c in range(nchip) for k in range(2)])

    def cross(n):
        return perm([(dev(c, k), dev(c + n, 1 - k)) for c in range(nchip) for k in range(2)])

    send_o = [
        perm([(dev(c, 0), dev(c + 2, 0)) for c in range(nchip)] + [(dev(c, 1), dev(c - 2, 1)) for c in range(nchip)]),
        perm([(dev(c, 0), dev(c - 2, 1)) for c in range(nchip)] + [(dev(c, 1), dev(c + 2, 0)) for c in range(nchip)]),
        chips(-1), cross(-1), chips(1), cross(1), lambda a: a, cross(0),
    ]

    def local(x, g, wqkv, wo):
        t, d = x.shape
        _, _, nh, dh = wqkv.shape
        hw = dh // 2
        ng = nchip // 2
        hc = nh // 2
        hl = hc // ng
        me = lax.axis_index("seq")
        chip, core = me // 2, me % 2
        grp = chip % ng
        i32 = lambda *v: jnp.stack([jnp.asarray(a, jnp.int32) for a in v])
        nj = 2
        r = t // nj

        xn = []
        for j in range(nj):
            xf = x[j * r:(j + 1) * r].astype(F32)
            xn.append((xf * lax.rsqrt(jnp.mean(xf * xf, axis=-1, keepdims=True) + 1e-5) * g).astype(BF))

        inv = 10000.0 ** (-jnp.arange(hw, dtype=F32) * 2.0 / dh)
        ab = jnp.arange(t, dtype=F32)[:, None] * inv[None, :]
        ac = (jnp.arange(p, dtype=F32) * t)[:, None] * inv[None, :]
        cosb, sinb, cosc, sinc = jnp.cos(ab), jnp.sin(ab), jnp.cos(ac), jnp.sin(ac)

        wall = _weights(wqkv, core.astype(jnp.int32).reshape(1))

        xs = [[None] * nj for _ in range(5)]
        for j in range(nj):
            xs[2][j] = xn[j]
            xs[1][j] = chips(1)(xn[j])
            xs[3][j] = chips(-1)(xn[j])
            xs[0][j] = chips(1)(xs[1][j])
            xs[4][j] = chips(-1)(xs[3][j])
        xo = [[cross(0)(a) for a in row] for row in xs]

        def wi(kind, gg, h):
            return kind * hc + hl * (gg % ng) + h

        kv_shape = (5, hl, 2, 2, nj, r, dh)
        q_shape = (5, hl, 2, nj, r, dh)
        near = None

        def project_near(slot, j, near):
            rc = (chip + slot - 2 + nchip) % nchip
            full = slot not in (0, 4)
            half = 1 if slot == 0 else 0
            tiles = [(True, 1 + kv, 0, 0) for h in range(hl) for kv in range(2)] + [(full, 0, 1, 0) for h in range(hl)]
            widx = i32(*([wi(1 + kv, grp, h) for h in range(hl) for kv in range(2)] + [wi(0, grp, h) for h in range(hl)]))
            qblk = (1, 1, 2, 1, r, dh) if full else (1, 1, 1, 1, r, dh)
            outs = [
                (kv_shape, (1, 1, 1, 2, 1, r, dh), lambda s: (slot, s // 2, s % 2, 0, j, 0, 0)),
                (q_shape, qblk, lambda s: (slot, s, 0 if full else half, j, 0, 0)),
            ]
            return _project(i32(core, rc), widx, xs[slot][j], xo[slot][j], wall, cosb, sinb, cosc, sinc, tiles, outs, j, half, near)

        def project_far(slot, j):
            rc = (chip + slot - 2 + nchip) % nchip
            g1 = grp + 1 if slot == 0 else grp + ng - 1
            g2 = grp + 2
            half = 0 if slot == 0 else 1
            tiles = [(True, 1 + kv, h, 0) for h in range(hl) for kv in range(2)] + \
                    [(False, 1 + kv, hl + h, 0) for h in range(hl) for kv in range(2)]
            widx = i32(*[wi(1 + kv, gg, h) for gg in (g1, g2) for h in range(hl) for kv in range(2)])
            outs = [((2, 2, r, dh), (1, 2, r, dh), lambda s: (s, 0, 0, 0))] * hl + \
                   [((2, r, dh), (1, r, dh), lambda s: (s, 0, 0))] * hl
            o = _project(i32(core, rc), widx, xs[slot][j], xo[slot][j], wall, cosb, sinb, cosc, sinc, tiles, outs, j, half)
            return o[:hl], o[hl:]

        f1p = [[None] * nj for _ in range(hl)]
        f1m = [[None] * nj for _ in range(hl)]
        f2p = [[None] * nj for _ in range(hl)]
        f2m = [[None] * nj for _ in range(hl)]
        for j in range(nj):
            near = project_near(2, j, near)
        for j in range(nj):
            near = project_near(1, j, near)
            near = project_near(3, j, near)
        for j in range(nj):
            ap, bp = project_far(0, j)
            am, bm = project_far(4, j)
            for h in range(hl):
                f1p[h][j] = chips(1)(ap[h])
                f1m[h][j] = chips(-1)(am[h])
                f2p[h][j] = chips(2)(bp[h])
                f2m[h][j] = chips(-2)(bm[h])
            near = project_near(0, j, near)
            near = project_near(4, j, near)
        nkv, nq = near

        def ent(slot, kk):
            return [slot, kk, 2 * ((chip + slot - 2 + nchip) % nchip) + kk]
        far_a = [jnp.where(core == 0, a, b) for a, b in zip(ent(4, 0), ent(0, 1))]
        far_b = [jnp.where(core == 0, b, a) for a, b in zip(ent(4, 0), ent(0, 1))]
        tab = i32(chip, *far_a, *far_b, *ent(1, core), *ent(1, 1 - core), *ent(3, core), *ent(3, 1 - core),
                  *ent(2, core), *ent(2, 1 - core))
        heads_of = lambda gg, kk, h: hc * kk + hl * (gg % ng) + h

        y = x
        for h in range(hl):
            got = []
            for sel in ((0, 1, 2, 3), (4, 5, 6, 7)):
                o = _attend(tab, h, sel, nkv, nq, f1p[h], f1m[h], f2p[h], f2m[h])
                got += [send_o[e](a) for e, a in zip(sel, o)]
            heads = i32(*[heads_of(gg, kk, h) for gg in (grp + 2, grp + 1, grp + ng - 1, grp) for kk in (core, 1 - core)])
            y = _out_proj(heads, got, wo, y, F32 if h < hl - 1 else BF)
        return y

    return jax.shard_map(local, mesh=mesh,
                         in_specs=(rows, P(None), P(None, None, None, None), P(None, None, None)),
                         out_specs=rows, check_vma=False)
```

```python
import functools

import jax
import jax.numpy as jnp
import numpy as np
from jax import lax
from jax.experimental import pallas as pl
from jax.experimental.pallas import tpu as pltpu
from jax.sharding import PartitionSpec as P

BF = jnp.bfloat16
F32 = jnp.float32
I32 = jnp.int32
VMEM_LIMIT = 63 * 2**20
R = 256

OWN, N1A, N1B, FWA, N2A, FWB, N2B = range(7)


def _pick(i, values):
    out = jnp.asarray(values[0], I32)
    for n, v in enumerate(values[1:], 1):
        out = jnp.where(i == n, v, out)
    return out


def _mega_body(p, x_ref, g_ref, w_ref, cosb, sinb, cosc, sinc, o_ref, wall, xb,
               kvs, qs, xv, wt, sa, sb, acc, ms, ls, fb, ob, cs, sn, pin, pout,
               ld_sem, wt_sem, pi_sem, po_sem, xs_sem, xr_sem, fs_sem, fr_sem, os_sem, or_sem):
    nchip = p // 2
    ng = nchip // 2
    d = x_ref.shape[1]
    t_rows = x_ref.shape[0]
    hl = 2
    hc = hl * ng
    hw = R // 2
    me = lax.axis_index("seq")
    chip, core = lax.div(me, 2), lax.rem(me, 2)
    grp = lax.rem(chip, ng)

    def ring(off):
        return lax.rem(chip + off + nchip, nchip)

    def send(src, dst, ssem, rsem, off, other):
        k = jnp.where(other, 1 - core, core) if not isinstance(other, int) else (1 - core if other else core)
        return pltpu.make_async_remote_copy(src, dst, ssem, rsem, device_id={"seq": 2 * ring(off) + k},
                                            device_id_type=pl.DeviceIdType.MESH)

    barrier = pltpu.get_barrier_semaphore()
    peers = [(0, 1)] + [(o, k) for o in (1, -1, 2, -2) for k in (0, 1)]
    for o, k in peers:
        pl.semaphore_signal(barrier, inc=1, device_id={"seq": 2 * ring(o) + (1 - core if k else core)},
                            device_id_type=pl.DeviceIdType.MESH)

    def x_send(slot, j, to, other):
        src = xb.at[slot, j, 0]
        dst = xb.at[slot, j, 1] if other else xb.at[slot - to, j, 0]
        return send(src, dst, xs_sem.at[slot, j, 0 if other else (1 if to > 0 else 2)],
                    xr_sem.at[slot, j, 1] if other else xr_sem.at[slot - to, j, 0], to, other)

    def x_wait(slot, j, other):
        pltpu.make_async_copy(xb.at[slot, j, other], xb.at[slot, j, other], xr_sem.at[slot, j, other]).wait()

    for j in range(2):
        pltpu.make_async_copy(x_ref.at[pl.ds(j * R, R)], xv.at[j], ld_sem.at[j]).start()
    for j in range(2):
        pltpu.make_async_copy(x_ref.at[pl.ds(j * R, R)], xv.at[j], ld_sem.at[j]).wait()

        def norm(i, c):
            rows = pl.ds(i * 32, 32)
            xf = xv[j, rows, :].astype(F32)
            y = xf * lax.rsqrt(jnp.mean(xf * xf, axis=-1, keepdims=True) + 1e-5) * g_ref[...]
            xv[j, rows, :] = y.astype(BF)
            return c
        lax.fori_loop(0, R // 32, norm, 0)
        out = pltpu.make_async_copy(xv.at[j], xb.at[2, j, 0], ld_sem.at[2 + j])
        out.start()
        out.wait()
        if j == 0:
            pl.semaphore_wait(barrier, len(peers))
        x_send(2, j, 1, 0).start()
        x_send(2, j, -1, 0).start()
        x_send(2, j, 0, 1).start()

    nb = d // R

    def w_in(i):
        kind, b = lax.div(i, nb), lax.rem(i, nb)
        return pltpu.make_async_copy(w_ref.at[pl.ds(b * R, R), kind, pl.ds(pl.multiple_of(core * hc, hc), hc)],
                                     pin.at[lax.rem(i, 2)], pi_sem.at[lax.rem(i, 2)])

    def w_out(i):
        kind, b = lax.div(i, nb), lax.rem(i, nb)
        return pltpu.make_async_copy(pout.at[lax.rem(i, 2)], wall.at[pl.ds(kind * hc, hc), pl.ds(b * R, R)],
                                     po_sem.at[lax.rem(i, 2)])

    w_in(jnp.int32(0)).start()

    def prep(i, c):
        @pl.when(i + 1 < 3 * nb)
        def _():
            w_in(i + 1).start()
        w_in(i).wait()

        @pl.when(i >= 2)
        def _():
            w_out(i - 2).wait()
        pout[lax.rem(i, 2)] = jnp.swapaxes(pin[lax.rem(i, 2)], 0, 1)
        w_out(i).start()
        return c
    lax.fori_loop(0, 3 * nb, prep, 0)
    for e in (2, 1):
        w_out(jnp.int32(3 * nb - e)).wait()

    def f_of(st):
        f = lax.div(st, 2)
        return _pick(f, (0, 0, 0, 1, 1, 1)), _pick(f, (0, 0, 2, 0, 2, 2)), _pick(f, (1, 2, ng - 1, 1, ng - 1, 2))

    def is_fw(ph):
        return jnp.logical_or(ph == FWA, ph == FWB)

    def is_n2(ph):
        return jnp.logical_or(ph == N2A, ph == N2B)

    def head_of(ph, st):
        nh = lax.rem(st, 2)
        return jnp.where(jnp.logical_and(is_n2(ph), st >= 4), 1 - nh, nh)

    def widx(ph, st):
        fh, _, fg = f_of(st)
        near = _pick(lax.div(st, 2), (hc, 2 * hc, 0)) + hl * grp + head_of(ph, st)
        fwd = hc * (1 + lax.rem(st, 2)) + hl * lax.rem(grp + fg, ng) + fh
        return jnp.where(is_fw(ph), fwd, near)

    def w_load(ph, st, gs):
        return pltpu.make_async_copy(wall.at[widx(ph, st)], wt.at[lax.rem(gs, 2)], wt_sem.at[lax.rem(gs, 2)])

    def off_of(ph, m):
        a = jnp.where(ph == OWN, 0, jnp.where(ph <= N1B, 1, 2))
        return jnp.where(m < 2, -a, a)

    def chunk_of(ph, m):
        return jnp.where(ph == OWN, lax.div(m, 2), jnp.where(jnp.logical_or(ph == N1B, ph >= FWB), 1, 0))

    def x_load(ph, m):
        return pltpu.make_async_copy(xb.at[off_of(ph, m) + 2, chunk_of(ph, m), lax.rem(m, 2)], xv.at[m], ld_sem.at[m])

    def block_of(ph, m):
        return 2 * ring(off_of(ph, m)) + jnp.where(lax.rem(m, 2) == 0, core, 1 - core)

    def f_send(j, f):
        h, to = ((0, 1), (0, 2), (0, -1), (1, 1), (1, -1), (1, -2))[f]
        src_off = -2 if to > 0 else 2
        return send(fb.at[j, f], kvs.at[:, h, pl.ds(2 * ring(src_off), 2), j], fs_sem.at[j, f], fr_sem.at[j, f], to, 0)

    def f_wait(j, f):
        h, frm = ((0, -3), (0, 4), (0, 3), (1, -3), (1, 3), (1, 4))[f]
        ref = kvs.at[:, h, pl.ds(2 * ring(frm), 2), j]
        pltpu.make_async_copy(ref, ref, fr_sem.at[j, f]).wait()

    def phase(ph, gs):
        for at, j, slots in ((OWN, 0, (1, 3)), (N1B, 1, (1, 3))):
            @pl.when(ph == at)
            def _(j=j, slots=slots):
                for s in slots:
                    x_wait(s, j, 0)
                    x_send(s, j, 1 if s == 1 else -1, 0).start()
                    x_send(s, j, 0, 1).start()
        for at, j in ((FWA, 0), (FWB, 1)):
            @pl.when(ph == at)
            def _(j=j):
                for s in (0, 4):
                    x_wait(s, j, 0)
                    x_send(s, j, 0, 1).start()
        for at, waits in ((OWN, ((2, 0), (2, 1))), (N1A, ((1, 0), (3, 0))), (N1B, ((1, 1), (3, 1))),
                          (FWA, ((0, 0), (4, 0))), (FWB, ((0, 1), (4, 1)))):
            @pl.when(ph == at)
            def _(waits=waits):
                for s, j in waits:
                    x_wait(s, j, 1)

        @pl.when(jnp.logical_not(is_n2(ph)))
        def _():
            for m in range(4):
                x_load(ph, m).start()
                b = block_of(ph, jnp.int32(m))
                rows = pl.ds(pl.multiple_of(chunk_of(ph, jnp.int32(m)) * R, R), R)
                cc, sc = cosc[pl.ds(b, 1), :], sinc[pl.ds(b, 1), :]
                cb, sb_ = cosb[rows, :], sinb[rows, :]
                cs[m] = cb * cc - sb_ * sc
                sn[m] = sb_ * cc + cb * sc
            for m in range(4):
                x_load(ph, m).wait()

        fw = is_fw(ph)
        ns = jnp.where(fw, 12, 6)

        def step(st, gs):
            nxt_in = st + 1 < ns
            nph = jnp.where(nxt_in, ph, ph + 1)
            nst = jnp.where(nxt_in, st + 1, 0)

            @pl.when(nph <= N2B)
            def _():
                w_load(nph, nst, gs + 1).start()
            w_load(ph, st, gs).wait()
            kind = jnp.where(fw, 1 + lax.rem(st, 2), _pick(lax.div(st, 2), (1, 2, 0)))
            fh, flo, _ = f_of(st)
            n2q = jnp.logical_and(is_n2(ph), st >= 4)
            h = jnp.where(fw, fh, head_of(ph, st))
            lo = jnp.where(fw, flo, jnp.where(jnp.logical_and(n2q, st == 5), 2, 0))
            cnt = jnp.where(jnp.logical_or(fw, n2q), 1, 2)
            f = lax.div(st, 2)
            jf = jnp.where(ph == FWB, 1, 0)
            wslot = lax.rem(gs, 2)

            def dots(m):
                return [jnp.dot(xv[m + e], wt[wslot], preferred_element_type=F32) for e in range(2)]

            @pl.when(kind != 2)
            def _():
                scale = jnp.where(kind == 0, R ** -0.5, 1.0).astype(F32)

                def two(u, c):
                    m = lo + 2 * u
                    av = dots(m)
                    for e in range(2):
                        a = av[e] * scale
                        a1, a2 = a[:, :hw], a[:, hw:]
                        cv, sv = cs[m + e], sn[m + e]
                        a = jnp.concatenate([a1 * cv - a2 * sv, a2 * cv + a1 * sv], axis=-1).astype(BF)
                        blk = block_of(ph, m + e)
                        kk = lax.rem(blk, 2)
                        j = chunk_of(ph, m + e)

                        @pl.when(fw)
                        def _():
                            fb[jf, f, 0, kk] = a

                        @pl.when(jnp.logical_and(jnp.logical_not(fw), kind == 1))
                        def _():
                            kvs[0, h, blk, j] = a

                        @pl.when(kind == 0)
                        def _():
                            o = off_of(ph, m)
                            qi = jnp.where(o == 0, 6, jnp.where(o == -1, 2, jnp.where(o == 1, 4, 0))) + e
                            qs[h, qi, j] = a
                    return c
                lax.fori_loop(0, cnt, two, 0)

            @pl.when(kind == 2)
            def _():
                def two(u, c):
                    m = lo + 2 * u
                    av = dots(m)
                    for e in range(2):
                        a = av[e].astype(BF).T
                        blk = block_of(ph, m + e)
                        kk = lax.rem(blk, 2)
                        j = chunk_of(ph, m + e)

                        @pl.when(fw)
                        def _():
                            fb[jf, f, 1, kk] = a

                        @pl.when(jnp.logical_not(fw))
                        def _():
                            kvs[1, h, blk, j] = a
                    return c
                lax.fori_loop(0, cnt, two, 0)

            for n in range(3):
                @pl.when(jnp.logical_and(ph == FWA, st == 2 * n + 1))
                def _(n=n):
                    f_send(0, n).start()

                @pl.when(jnp.logical_and(ph == FWB, st == 2 * n + 1))
                def _(n=n):
                    f_send(1, n).start()
                    if n == 2:
                        for m in range(3, 6):
                            f_send(0, m).start()

                @pl.when(jnp.logical_and(ph == FWB, st == 2 * n + 7))
                def _(n=n):
                    f_send(1, n + 3).start()
            return gs + 1
        return lax.fori_loop(0, ns, step, gs)

    w_load(jnp.int32(OWN), jnp.int32(0), jnp.int32(0)).start()
    lax.fori_loop(0, N2B + 1, phase, jnp.int32(0))

    kb, qb = 4 * R, 2 * R

    def q_off(h, e):
        return jnp.where(e < 2, jnp.where(h == 0, 2, -2), jnp.where(e < 4, -1, jnp.where(e < 6, 1, 0)))

    def o_send(i):
        h, e = lax.div(i, 8), lax.rem(i, 8)
        return send(ob.at[i], o_ref.at[i], os_sem.at[i], or_sem.at[i], q_off(h, e), lax.rem(e, 2) == 1)

    def o_keep(i):
        return pltpu.make_async_copy(ob.at[i], o_ref.at[i], os_sem.at[i])

    def attend(i, c):
        h, e = lax.div(i, 8), lax.rem(i, 8)
        for hh in range(hl):
            @pl.when(i == 8 * hh)
            def _(hh=hh):
                for j in range(2):
                    for n in range(3):
                        f_wait(j, 3 * hh + n)
        pb = 2 * ring(q_off(h, e)) + jnp.where(lax.rem(e, 2) == 0, core, 1 - core)
        acc[...] = jnp.zeros_like(acc)
        ms[...] = jnp.full_like(ms, -jnp.inf)
        ls[...] = jnp.zeros_like(ls)

        def scores(n, dst):
            kblk = kvs[0, h, pl.ds(2 * n, 2)].reshape(kb, R)
            q = qs[h, e].reshape(qb, R)
            dst[...] = lax.dot_general(kblk, q, (((1,), (1,)), ((), ())), preferred_element_type=F32)

        def update(n, src, masked):
            s = src[...]
            if masked:
                kp = n * kb + lax.broadcasted_iota(I32, (kb, qb), 0)
                qp = pb * qb + lax.broadcasted_iota(I32, (kb, qb), 1)
                s = jnp.where(qp >= kp, s, -jnp.inf)
            mo = ms[...]
            mn = jnp.maximum(mo, jnp.max(s, axis=0, keepdims=True))
            al = jnp.exp(mo - mn)
            pr = jnp.exp(s - mn)
            ls[...] = ls[...] * al + jnp.sum(pr, axis=0, keepdims=True)
            ms[...] = mn
            vblk = kvs[1, h, pl.ds(2 * n, 2)]
            vblk = jnp.concatenate([vblk[a, b] for a in range(2) for b in range(2)], axis=-1)
            acc[...] = acc[...] * al + jnp.dot(vblk, pr.astype(BF), preferred_element_type=F32)

        nf = lax.div(pb, 2)
        scores(0, sa)

        def two(u, c):
            n = 2 * u
            scores(n + 1, sb)
            update(n, sa, False)
            scores(n + 2, sa)
            update(n + 1, sb, False)
            return c
        lax.fori_loop(0, lax.div(nf, 2), two, 0)

        @pl.when(lax.rem(nf, 2) == 1)
        def _():
            scores(nf, sb)
            update(nf - 1, sa, False)
            update(nf, sb, True)

        @pl.when(lax.rem(nf, 2) == 0)
        def _():
            update(nf, sa, True)
        ob[i] = (acc[...] / ls[...]).T.astype(BF)

        @pl.when(e == 6)
        def _():
            o_keep(i).start()

        @pl.when(e != 6)
        def _():
            o_send(i).start()
        return c
    lax.fori_loop(0, 8 * hl, attend, 0)

    for j in range(2):
        for s in range(5):
            x_send(s, j, 0, 1).wait_send()
        for s, to in ((2, 1), (2, -1), (1, 1), (3, -1)):
            x_send(s, j, to, 0).wait_send()
        for f in range(6):
            f_send(j, f).wait_send()

    def drain(i, c):
        @pl.when(lax.rem(i, 8) == 6)
        def _():
            o_keep(i).wait()

        @pl.when(lax.rem(i, 8) != 6)
        def _():
            o_send(i).wait()
        return c
    lax.fori_loop(0, 8 * hl, drain, 0)


def _mega(x, g, wqkv, p):
    t, d = x.shape
    _, _, nh, dh = wqkv.shape
    hw = dh // 2
    nchip = p // 2
    hc = nh // 2
    inv = 10000.0 ** (-np.arange(hw) * 2.0 / dh)
    ab, ac = np.arange(t)[:, None] * inv, (np.arange(p) * t)[:, None] * inv
    rot = [jnp.asarray(f(a), F32) for a in (ab, ac) for f in (np.cos, np.sin)]
    any_ = pl.BlockSpec(memory_space=pl.ANY)
    vm = pl.BlockSpec(memory_space=pltpu.VMEM)
    dma = pltpu.SemaphoreType.DMA
    return pl.pallas_call(
        functools.partial(_mega_body, p),
        in_specs=[any_, vm, any_, vm, vm, vm, vm],
        out_specs=[any_, any_, any_],
        out_shape=[jax.ShapeDtypeStruct((16, t, dh), BF), jax.ShapeDtypeStruct((3 * hc, d, dh), BF),
                   jax.ShapeDtypeStruct((5, 2, 2, R, d), BF)],
        scratch_shapes=[
            pltpu.VMEM((2, 2, 2 * nchip, 2, R, R), BF), pltpu.VMEM((2, 8, 2, R, R), BF), pltpu.VMEM((4, R, d), BF),
            pltpu.VMEM((2, d, R), BF), pltpu.VMEM((4 * R, 2 * R), F32), pltpu.VMEM((4 * R, 2 * R), F32),
            pltpu.VMEM((R, 2 * R), F32), pltpu.VMEM((1, 2 * R), F32), pltpu.VMEM((1, 2 * R), F32),
            pltpu.VMEM((2, 6, 2, 2, R, R), BF), pltpu.VMEM((16, 2 * R, R), BF), pltpu.VMEM((4, R, hw), F32),
            pltpu.VMEM((4, R, hw), F32), pltpu.VMEM((2, R, hc, dh), BF), pltpu.VMEM((2, hc, R, dh), BF),
            dma((4,)), dma((2,)), dma((2,)), dma((2,)), dma((5, 2, 3)), dma((5, 2, 2)), dma((2, 6)), dma((2, 6)),
            dma((16,)), dma((16,))],
        compiler_params=pltpu.CompilerParams(vmem_limit_bytes=VMEM_LIMIT, collective_id=0, has_side_effects=True),
        name="qkv_attend",
    )(x, g.reshape(1, d), wqkv, rot[0], rot[1], rot[2], rot[3])[0]


def _out_proj(heads, o, wo, res):
    n, qb, dh = o.shape
    dm = wo.shape[-1]
    bn = 512

    def body(h_ref, o_ref, *refs):
        w, res_ref, y_ref = refs[:n], refs[n], refs[n + 1]
        a = res_ref[...].astype(F32)
        for i in range(n):
            a = a + jnp.dot(o_ref[i], w[i][0], preferred_element_type=F32)
        y_ref[...] = a.astype(BF)

    return pl.pallas_call(
        body,
        grid_spec=pltpu.PrefetchScalarGridSpec(
            num_scalar_prefetch=1, grid=(dm // bn,),
            in_specs=[pl.BlockSpec((n, qb, dh), lambda c, h: (0, 0, 0))]
            + [pl.BlockSpec((1, dh, bn), functools.partial(lambda i, c, h: (h[i], 0, c), i)) for i in range(n)]
            + [pl.BlockSpec((qb, bn), lambda c, h: (0, c))],
            out_specs=pl.BlockSpec((qb, bn), lambda c, h: (0, c))),
        out_shape=jax.ShapeDtypeStruct((qb, dm), BF),
        compiler_params=pltpu.CompilerParams(vmem_limit_bytes=VMEM_LIMIT),
        name="out_proj",
    )(heads, o, *([wo] * n), res)


def solution(mesh):
    p = mesh.shape["seq"]
    rows = P(("data", "seq"), None)
    nchip = p // 2

    def local(x, g, wqkv, wo):
        _, _, nh, dh = wqkv.shape
        ng = nchip // 2
        hc = nh // 2
        hl = hc // ng
        me = lax.axis_index("seq")
        chip, core = me // 2, me % 2
        grp = chip % ng
        o = _mega(x, g, wqkv, p)
        heads = jnp.stack([jnp.asarray(hc * kk + hl * (gg % ng) + h, I32)
                           for h in range(hl) for gg in (grp + 2, grp + 1, grp + ng - 1, grp) for kk in (core, 1 - core)])
        return _out_proj(heads, o, wo, x)

    return jax.shard_map(local, mesh=mesh,
                         in_specs=(rows, P(None), P(None, None, None, None), P(None, None, None)),
                         out_specs=rows, check_vma=False)
```

```python
import functools

import jax
import jax.numpy as jnp
import numpy as np
from jax import lax
from jax.experimental import pallas as pl
from jax.experimental.pallas import tpu as pltpu
from jax.sharding import PartitionSpec as P

BF = jnp.bfloat16
F32 = jnp.float32
I32 = jnp.int32
VMEM_LIMIT = 63 * 2**20
R = 256

OWN, N1A, N1B, FWA, N2A, FWB, N2B = range(7)


TWO = range(2)


def _loop(n, body):
    return lax.fori_loop(0, n, body, 0)


def _odd(a):
    return lax.rem(a, 2)


def _half(a):
    return lax.div(a, 2)


def _rem3(a):
    return lax.rem(a, 3)


def _rem8(a):
    return lax.rem(a, 8)


def _div8(a):
    return lax.div(a, 8)


def _pick(i, values):
    out = jnp.asarray(values[0], I32)
    for n, v in enumerate(values[1:], 1):
        out = jnp.where(i == n, v, out)
    return out


def _body(p, x_ref, g_ref, w_ref, wo_ref, cosb, sinb, cosc, sinc, y_ref, wall, xb, kvs, qs, fb, ob, og,
          sa, sb, acc, ms, ls, ld_sem, wt_sem, wo_sem, xs_sem, xr_sem, fs_sem, fr_sem, os_sem, or_sem):
    nchip = p // 2
    ng = nchip // 2
    d = x_ref.shape[1]
    hl = 2
    hc = hl * ng
    hw = R // 2
    me = lax.axis_index("seq")
    chip, core = _half(me), _odd(me)
    grp = lax.rem(chip, ng)

    def ring(off):
        return lax.rem(chip + off + nchip, nchip)

    def send(src, dst, ssem, rsem, off, other):
        k = jnp.where(other, 1 - core, core) if not isinstance(other, int) else (1 - core if other else core)
        return pltpu.make_async_remote_copy(src, dst, ssem, rsem, device_id={"seq": 2 * ring(off) + k},
                                            device_id_type=pl.DeviceIdType.MESH)

    barrier = pltpu.get_barrier_semaphore()
    peers = [(0, 1)] + [(o, k) for o in (1, -1, 2, -2) for k in (0, 1)]
    for o, k in peers:
        pl.semaphore_signal(barrier, inc=1, device_id={"seq": 2 * ring(o) + (1 - core if k else core)},
                            device_id_type=pl.DeviceIdType.MESH)

    def x_send(slot, j, to, other):
        src = x_ref.at[pl.ds(0, R)] if (slot, j) == (2, 0) else xb.at[slot, j, 0]
        dst = xb.at[slot, j, 1] if other else xb.at[slot - to, j, 0]
        return send(src, dst, xs_sem.at[slot, j, 0 if other else (1 if to > 0 else 2)],
                    xr_sem.at[slot, j, 1] if other else xr_sem.at[slot - to, j, 0], to, other)

    def x_wait(slot, j, other):
        pltpu.make_async_copy(xb.at[slot, j, other], xb.at[slot, j, other], xr_sem.at[slot, j, other]).wait()

    nb = d // R

    def norm(ref):
        def rows32(i, c):
            rows = pl.ds(i * 32, 32)
            xf = ref[rows, :].astype(F32)
            y = xf * lax.rsqrt(jnp.mean(xf * xf, axis=-1, keepdims=True) + 1e-5) * g_ref[...]
            ref[rows, :] = y.astype(BF)
            return c
        _loop(R // 32, rows32)

    def start(xv, pin, pout):
        x1 = pltpu.make_async_copy(x_ref.at[pl.ds(R, R)], xv, ld_sem.at[0])
        x1.start()
        pl.semaphore_wait(barrier, len(peers))
        for to, other in ((1, 0), (-1, 0), (0, 1)):
            x_send(2, 0, to, other).start()
        x1.wait()
        norm(xv)
        out = pltpu.make_async_copy(xv, xb.at[2, 1, 0], ld_sem.at[1])
        out.start()
        out.wait()
        for to, other in ((1, 0), (-1, 0), (0, 1)):
            x_send(2, 1, to, other).start()

        def w_in(i):
            kind, b = _rem3(lax.div(i, nb) + 1), lax.rem(i, nb)
            return pltpu.make_async_copy(w_ref.at[pl.ds(b * R, R), kind, pl.ds(pl.multiple_of(core * hc, hc), hc)],
                                         pin.at[_odd(i)], wt_sem.at[_odd(i)])

        def kv_out(i):
            kind, b = lax.div(i, nb) + 1, lax.rem(i, nb)
            return pltpu.make_async_copy(pout.at[_odd(i)], wall.at[pl.ds(kind * hc, hc), pl.ds(b * R, R)],
                                         ld_sem.at[_odd(i)])

        def q_out(i):
            return pltpu.make_async_copy(pout.at[_odd(i), pl.ds(0, hl)],
                                         wall.at[pl.ds(hl * grp, hl), pl.ds(lax.rem(i, nb) * R, R)], ld_sem.at[_odd(i)])

        def put_kv(i):
            pout[_odd(i)] = jnp.swapaxes(pin[_odd(i)], 0, 1)

        def put_q(i):
            for gv in range(ng):
                @pl.when(grp == gv)
                def _(gv=gv):
                    pout[_odd(i), :hl] = jnp.swapaxes(pin[_odd(i), :, hl * gv:hl * gv + hl], 0, 1)

        def prep(put, out, lo, i, c):
            @pl.when(i + 1 < 3 * nb)
            def _():
                w_in(i + 1).start()
            w_in(i).wait()

            @pl.when(i >= lo + 2)
            def _():
                out(i - 2).wait()
            put(i)
            out(i).start()
            return c
        w_in(jnp.int32(0)).start()
        for put, out, lo, hi in ((put_kv, kv_out, 0, 2 * nb), (put_q, q_out, 2 * nb, 3 * nb)):
            lax.fori_loop(lo, hi, functools.partial(prep, put, out, lo), 0)
            for e in (2, 1):
                out(jnp.int32(hi - e)).wait()

    pl.run_scoped(start, pltpu.VMEM((R, d), BF), pltpu.VMEM((2, R, hc, R), BF), pltpu.VMEM((2, hc, R, R), BF))

    even = _odd(chip) == 0

    kb, qb = 4 * R, 2 * R
    EARLY, NEAR, HEAD0, FAR = range(4)

    def q_off(e):
        return jnp.where(e < 2, jnp.where(even, 2, -2), jnp.where(e < 4, -1, jnp.where(e < 6, 1, 0)))

    def o_send(i):
        e = _rem8(i)
        return send(ob.at[i], og.at[i], os_sem.at[i], or_sem.at[i], q_off(e), _odd(e) == 1)

    def around(reach):
        b = ring(-reach)
        wrapped = jnp.logical_or(chip < reach, chip + reach >= nchip)
        return jnp.where(wrapped, ring(reach + 1), 0), b

    def attend(ps, e):
        h = jnp.where(ps == HEAD0, 0, 1)
        i = 8 * h + e
        qc = ring(q_off(e))
        pb = 2 * qc + jnp.where(_odd(e) == 0, core, 1 - core)
        w1, b1 = around(1)
        w2, b2 = around(2)
        rest = jnp.logical_and(ps == NEAR, e >= 2)
        up2 = ring(2)
        low_ok, up_ok = b2 < qc, up2 < qc
        n0 = jnp.where(ps == FAR, w2, jnp.where(rest, b2, 0))
        n1 = jnp.where(ps == EARLY, b1, jnp.where(rest, up2, b2))
        w = jnp.where(ps == EARLY, w1, jnp.where(rest, jnp.where(low_ok, 1, 0), jnp.where(ps == NEAR, w2, nchip)))
        cnt = jnp.where(
            ps == EARLY, jnp.where(qc >= b1, w1 + qc - b1, qc),
            jnp.where(rest, jnp.where(low_ok, 1, 0) + jnp.where(up_ok, 1, 0),
                      jnp.where(ps == NEAR, jnp.where(qc >= b2, w2 + qc - b2, qc),
                                jnp.where(ps == HEAD0, qc, jnp.where(qc >= b2, b2 - w2, 0)))))
        last = jnp.logical_not(jnp.logical_or(rest, ps == FAR))
        sl = jnp.where(ps == HEAD0, 8, e)

        def keys_of(idx):
            return jnp.where(idx >= cnt, qc, jnp.where(idx < w, n0 + idx, n1 + idx - w))

        @pl.when(last)
        def _():
            acc[sl] = jnp.zeros((R, qb), F32)
            ms[sl] = jnp.full((1, qb), -jnp.inf, F32)
            ls[sl] = jnp.zeros((1, qb), F32)

        def scores(idx, dst):
            n = keys_of(idx)
            kblk = kvs[0, h, pl.ds(2 * n, 2)].reshape(kb, R)
            q = qs[h, e].reshape(qb, R)
            s = lax.dot_general(kblk, q, (((1,), (1,)), ((), ())), preferred_element_type=F32)
            dst[...] = s.reshape(dst.shape)

        def update(idx, src, masked, nk=4):
            n = keys_of(idx)
            s = src[:nk].reshape(nk * R, qb)
            if masked:
                kp = n * kb + lax.broadcasted_iota(I32, s.shape, 0)
                qp = pb * qb + lax.broadcasted_iota(I32, s.shape, 1)
                s = jnp.where(qp >= kp, s, -jnp.inf)
            mo = ms[sl]
            mn = jnp.maximum(mo, jnp.max(s, axis=0, keepdims=True))
            al = jnp.exp(mo - mn)
            pr = jnp.exp(s - mn)
            ls[sl] = ls[sl] * al + jnp.sum(pr, axis=0, keepdims=True)
            ms[sl] = mn
            vblk = kvs[1, h, pl.ds(2 * n, 2)]
            vblk = jnp.concatenate([vblk[a // 2, a % 2] for a in range(nk)], axis=-1)
            acc[sl] = acc[sl] * al + jnp.dot(vblk, pr.astype(BF), preferred_element_type=F32)

        @pl.when(jnp.logical_or(cnt > 0, last))
        def _():
            scores(0, sa)

            def two(u, c2):
                scores(2 * u + 1, sb)
                update(2 * u, sa, False)
                scores(2 * u + 2, sa)
                update(2 * u + 1, sb, False)
                return c2
            _loop(_half(cnt), two)
            odd = _odd(cnt) == 1

            @pl.when(jnp.logical_and(odd, last))
            def _():
                scores(cnt, sb)
                update(cnt - 1, sa, False)

            @pl.when(jnp.logical_and(odd, jnp.logical_not(last)))
            def _():
                update(cnt - 1, sa, False)

            for buf, par in ((sa, 0), (sb, 1)):
                for kk in TWO:
                    @pl.when(jnp.logical_and(last, jnp.logical_and(_odd(cnt) == par, _odd(pb) == kk)))
                    def _(buf=buf, kk=kk):
                        update(cnt, buf, True, 2 + 2 * kk)

        @pl.when(ps >= HEAD0)
        def _():
            out = (acc[sl] / ls[sl]).T.astype(BF)

            @pl.when(e == 6)
            def _():
                og[i] = out

            @pl.when(e != 6)
            def _():
                ob[i] = out

    def f_wait_head(hh):
        for j in TWO:
            for n in range(3):
                f_wait(j, 3 * hh + n)

    def attend_loop():
        busy = chip >= ng

        def send_head0(n):
            for k in range(n):
                o_send(jnp.int32(k)).start()

        def one(it, c):
            ps, e = 1 + _div8(it), _rem8(it)

            @pl.when(it == 8)
            def _():
                f_wait_head(0)

            @pl.when(it == 16)
            def _():
                f_wait_head(1)

            @pl.when(jnp.logical_and(it == 16, jnp.logical_not(busy)))
            def _():
                send_head0(6)
                o_send(jnp.int32(7)).start()
            attend(ps, e)

            @pl.when(jnp.logical_and(ps == FAR, e != 6))
            def _():
                o_send(8 + e).start()

            @pl.when(jnp.logical_and(busy, it == 14))
            def _():
                send_head0(6)

            @pl.when(jnp.logical_and(busy, it == 15))
            def _():
                o_send(e).start()
            return c
        _loop(24, one)

    def f_of(ph, st):
        f = _half(st)
        n = _rem3(f)
        return lax.div(f, 3), jnp.where(n == 1, jnp.where(ph == FWA, 0, 2), n), _pick(n, (1, 2, ng - 1))

    def is_fw(ph):
        return jnp.logical_or(ph == FWA, ph == FWB)

    def is_n2(ph):
        return jnp.logical_or(ph == N2A, ph == N2B)

    def head_of(ph, st):
        return _odd(st)

    def widx(ph, st):
        fh, _, fg = f_of(ph, st)
        near = _pick(_half(st), (hc, 2 * hc, 0)) + hl * grp + head_of(ph, st)
        fwd = hc * (1 + _odd(st)) + hl * lax.rem(grp + fg, ng) + fh
        return jnp.where(is_fw(ph), fwd, near)

    def w_load(wt, ph, st, gs):
        return pltpu.make_async_copy(wall.at[widx(ph, st)], wt.at[_rem3(gs)], wt_sem.at[_rem3(gs)])

    def steps_of(ph):
        return jnp.where(is_fw(ph), 12, 6)

    def next_step(ph, st):
        inside = st + 1 < steps_of(ph)
        return jnp.where(inside, ph, ph + 1), jnp.where(inside, st + 1, 0)

    def off_of(ph, m):
        a = jnp.where(ph == OWN, 0, jnp.where(ph <= N1B, 1, 2))
        return jnp.where(m < 2, -a, a)

    def chunk_of(ph, m):
        return jnp.where(ph == OWN, _half(m), jnp.where(jnp.logical_or(ph == N1B, ph >= FWB), 1, 0))

    def x_load(xv, ph, m):
        return pltpu.make_async_copy(xb.at[off_of(ph, m) + 2, chunk_of(ph, m), _odd(m)], xv.at[m], ld_sem.at[m])

    def block_of(ph, m):
        return 2 * ring(off_of(ph, m)) + jnp.where(_odd(m) == 0, core, 1 - core)

    def f_send(j, f):
        h, to = f // 3, (1, (2, -2)[j], -1)[f % 3]
        src_off = -2 if to > 0 else 2
        return send(fb.at[j, f], kvs.at[:, h, pl.ds(2 * ring(src_off), 2), j], fs_sem.at[j, f], fr_sem.at[j, f], to, 0)

    def f_wait(j, f):
        h, frm = f // 3, (-3, 4, 3)[f % 3]
        ref = kvs.at[:, h, pl.ds(2 * ring(frm), 2), j]
        pltpu.make_async_copy(ref, ref, fr_sem.at[j, f]).wait()

    def phase(xv, wt, cs, sn, res, ph, gs):
        def relay(j):
            for s in (1, 3):
                x_wait(s, j, 0)
                x_send(s, j, 1 if s == 1 else -1, 0).start()
                x_send(s, j, 0, 1).start()

        @pl.when(ph == OWN)
        def _():
            relay(0)

        @pl.when(ph == FWA)
        def _():
            def early(e, c):
                attend(jnp.int32(EARLY), e)
                return c
            lax.fori_loop(2, 8, early, 0)
        def share(j):
            for s in (0, 4):
                x_wait(s, j, 0)
                x_send(s, j, 0, 1).start()

        @pl.when(ph == FWA)
        def _():
            share(0)
        fw = is_fw(ph)
        raw = jnp.logical_or(ph == N1A, ph == FWA)

        def norms(lo, step=1):
            lax.fori_loop(0, 2, lambda m, c: (norm(xv.at[lo + step * m]), c)[1], 0)
        fresh = jnp.logical_not(is_n2(ph))

        @pl.when(fresh)
        def _():
            @pl.when(ph == OWN)
            def _():
                pltpu.make_async_copy(x_ref.at[pl.ds(0, R)], xv.at[0], ld_sem.at[0]).start()

            @pl.when(ph != OWN)
            def _():
                x_load(xv, ph, 0).start()
            x_load(xv, ph, 2).start()
            for m in range(4):
                b = block_of(ph, jnp.int32(m))
                rows = pl.ds(pl.multiple_of(chunk_of(ph, jnp.int32(m)) * R, R), R)
                cc, sc = cosc[pl.ds(b, 1), :], sinc[pl.ds(b, 1), :]
                cb, sb_ = cosb[rows, :], sinb[rows, :]
                cs[m] = cb * cc - sb_ * sc
                sn[m] = sb_ * cc + cb * sc
        @pl.when(raw)
        def _():
            for m in (0, 2):
                x_load(xv, ph, m).wait()
            norms(0, 2)
        for at, waits in ((OWN, ((2, 0), (2, 1))), (N1A, ((1, 0), (3, 0))), (N1B, ((1, 1), (3, 1))),
                          (FWA, ((0, 0), (4, 0))), (FWB, ((0, 1), (4, 1)))):
            @pl.when(ph == at)
            def _(waits=waits):
                for s, j in waits:
                    x_wait(s, j, 1)

        @pl.when(fresh)
        def _():
            for m in (1, 3):
                x_load(xv, ph, m).start()

        @pl.when(raw)
        def _():
            for m in (1, 3):
                x_load(xv, ph, m).wait()
            norms(1, 2)

        @pl.when(jnp.logical_and(fresh, jnp.logical_not(raw)))
        def _():
            for m in TWO:
                x_load(xv, ph, m).wait()

        @pl.when(ph == OWN)
        def _():
            norms(0)

        @pl.when(jnp.logical_or(ph == OWN, ph == N1B))
        def _():
            for m in (2, 3):
                x_load(xv, ph, m).wait()

        def step(st, gs):
            nph, nst = next_step(*next_step(ph, st))

            @pl.when(nph <= N2B)
            def _():
                w_load(wt, nph, nst, gs + 2).start()

            @pl.when(jnp.logical_and(ph == N1A, st == 4))
            def _():
                relay(1)

            @pl.when(jnp.logical_and(ph == N2A, st == 5))
            def _():
                share(1)

            @pl.when(jnp.logical_and(ph == FWB, st == 2))
            def _():
                for m in (2, 3):
                    x_load(xv, ph, m).wait()
            w_load(wt, ph, st, gs).wait()
            kind = jnp.where(fw, 1 + _odd(st), _pick(_half(st), (1, 2, 0)))
            fh, flo, _ = f_of(ph, st)
            n2q = jnp.logical_and(is_n2(ph), st >= 4)
            h = jnp.where(fw, fh, head_of(ph, st))
            lo = jnp.where(fw, flo, jnp.where(jnp.logical_and(n2q, even), 2, 0))
            cnt = jnp.where(jnp.logical_or(fw, n2q), 1, 2)
            f = _half(st)
            jf = jnp.where(ph == FWB, 1, 0)
            wslot = _rem3(gs)

            def dots(m):
                return [jnp.dot(xv[m + e], wt[wslot], preferred_element_type=F32) for e in TWO]

            @pl.when(kind != 2)
            def _():
                scale = jnp.where(kind == 0, R ** -0.5, 1.0).astype(F32)

                def two(u, c):
                    m = lo + 2 * u
                    av = dots(m)
                    for e in TWO:
                        a = av[e] * scale
                        a1, a2 = a[:, :hw], a[:, hw:]
                        cv, sv = cs[m + e], sn[m + e]
                        res[m + e] = jnp.concatenate([a1 * cv - a2 * sv, a2 * cv + a1 * sv], axis=-1).astype(BF)
                    return c
                _loop(cnt, two)

            @pl.when(kind == 2)
            def _():
                def two(u, c):
                    m = lo + 2 * u
                    av = dots(m)
                    for e in TWO:
                        res[m + e] = av[e].astype(BF).T
                    return c
                _loop(cnt, two)

            def put(m, c):
                blk = block_of(ph, m)
                j = chunk_of(ph, m)

                @pl.when(fw)
                def _():
                    fb[jf, f, kind - 1, _odd(blk)] = res[m]

                @pl.when(jnp.logical_and(jnp.logical_not(fw), kind > 0))
                def _():
                    kvs[kind - 1, h, blk, j] = res[m]

                @pl.when(kind == 0)
                def _():
                    o = off_of(ph, m)
                    qi = jnp.where(o == 0, 6, jnp.where(o == -1, 2, jnp.where(o == 1, 4, 0))) + _odd(m)
                    qs[h, qi, j] = res[m]
                return c
            lax.fori_loop(lo, lo + 2 * cnt, put, 0)

            for n in range(3):
                @pl.when(jnp.logical_and(ph == FWA, st == 2 * n + 1))
                def _(n=n):
                    f_send(0, n).start()

                @pl.when(jnp.logical_and(ph == FWB, st == 2 * n + 1))
                def _(n=n):
                    f_send(1, n).start()
                    if n == 0:
                        for m in (3, 4):
                            f_send(0, m).start()

                if n == 2:
                    @pl.when(jnp.logical_and(ph == FWA, st == 11))
                    def _():
                        f_send(0, 5).start()

                @pl.when(jnp.logical_and(ph == FWB, st == 2 * n + 7))
                def _(n=n):
                    f_send(1, n + 3).start()
            return gs + 1
        return lax.fori_loop(0, steps_of(ph), step, gs)

    def project(xv, wt, cs, sn, res):
        for n in TWO:
            w_load(wt, jnp.int32(OWN), jnp.int32(n), jnp.int32(n)).start()
        lax.fori_loop(0, N2B + 1, functools.partial(phase, xv, wt, cs, sn, res), jnp.int32(0))

    pl.run_scoped(project, pltpu.VMEM((4, R, d), BF), pltpu.VMEM((3, d, R), BF), pltpu.VMEM((4, R, hw), F32),
                  pltpu.VMEM((4, R, hw), F32), pltpu.VMEM((4, R, R), BF))

    attend_loop()

    dm = wo_ref.shape[2]
    nw = dm // 2
    cw = 2 * R
    ncol = nw // cw
    groups = ((0, 1, 2, 3), (4, 5, 6, 7), (8, 9, 14, 15), (10, 12), (11, 13))

    def piece(n, k):
        return _pick(n, [gr[k] if k < len(gr) else gr[0] for gr in groups])

    def wo_load(wv, n, half, ks):
        sl, out = _rem3(2 * n + half), []
        for k in ks:
            i = piece(n, k)
            gg = lax.rem(grp + _pick(_half(_rem8(i)), (2, 1, ng - 1, 0)), ng)
            head = hc * jnp.where(_odd(i) == 0, core, 1 - core) + hl * gg + _div8(i)
            out.append(pltpu.make_async_copy(wo_ref.at[head, :, pl.ds(half * nw, nw)], wv.at[sl, k], wo_sem.at[sl, k]))
        return out

    def wo_start(wv, n, half):
        @pl.when(n < len(groups))
        def _():
            for cp in wo_load(wv, n, half, (0, 1)):
                cp.start()

        @pl.when(n < 3)
        def _():
            for cp in wo_load(wv, n, half, (2, 3)):
                cp.start()

    def finish(yb, wv):
        res = pltpu.make_async_copy(x_ref, yb, wt_sem.at[1])
        res.start()
        for half in TWO:
            wo_start(wv, jnp.int32(0), half)
        res.wait()
        tops = (sa, sb)

        for half in TWO:
            def fill(i, c, half=half):
                to = pl.ds(pl.multiple_of(half * nw + i * cw, cw), cw)
                tops[half][i] = yb[:R, to].astype(F32)
                acc[half * ncol + i] = yb[R:, to].astype(F32)
                return c
            _loop(ncol, fill)

        def out(size, n, c):
            for half in TWO:
                sl = _rem3(2 * n + half)
                wo_start(wv, n + 1, half)
                if half == 0:
                    for k in range(size):
                        i = piece(n, k)

                        @pl.when(_rem8(i) != 6)
                        def _(i=i):
                            o_send(i).wait()
                for cp in wo_load(wv, n, half, range(size)):
                    cp.wait()
                oo = jnp.concatenate([og[piece(n, k)] for k in range(size)], axis=-1)

                def cols(i, c2, half=half, sl=sl, oo=oo):
                    at = pl.ds(pl.multiple_of(i * cw, cw), cw)
                    ww = jnp.concatenate([wv[sl, k, :, at] for k in range(size)], axis=0)
                    a = jnp.dot(oo, ww, preferred_element_type=F32)
                    tops[half][i] = tops[half][i] + a[:R]
                    acc[half * ncol + i] = acc[half * ncol + i] + a[R:]
                    return c2
                _loop(ncol, cols)

                if size == 2:
                    @pl.when(n == len(groups) - 1)
                    def _(half=half):
                        def store(i, c2):
                            to = pl.ds(pl.multiple_of(half * nw + i * cw, cw), cw)
                            yb[:R, to] = tops[half][i].astype(BF)
                            yb[R:, to] = acc[half * ncol + i].astype(BF)
                            pltpu.make_async_copy(yb.at[:, to], y_ref.at[:, to], wt_sem.at[0]).start()
                            return c2
                        _loop(ncol, store)
            return c
        _loop(3, functools.partial(out, 4))
        lax.fori_loop(3, len(groups), functools.partial(out, 2), 0)
        pltpu.make_async_copy(yb, y_ref, wt_sem.at[0]).wait()

    pl.run_scoped(finish, pltpu.VMEM((qb, dm), BF), pltpu.VMEM((3, 4, R, nw), BF))

    for j in TWO:
        for s in range(5):
            x_send(s, j, 0, 1).wait_send()
        for s, to in ((2, 1), (2, -1), (1, 1), (3, -1)):
            x_send(s, j, to, 0).wait_send()
        for f in range(6):
            f_send(j, f).wait_send()


def _sublayer(x, g, wqkv, wo, p):
    t, d = x.shape
    _, _, nh, dh = wqkv.shape
    hw = dh // 2
    nchip = p // 2
    hc = nh // 2
    inv = 10000.0 ** (-np.arange(hw) * 2.0 / dh)
    ab, ac = np.arange(t)[:, None] * inv, (np.arange(p) * t)[:, None] * inv
    rot = [jnp.asarray(f(a), F32) for a in (ab, ac) for f in (np.cos, np.sin)]
    any_ = pl.BlockSpec(memory_space=pl.ANY)
    vm = pl.BlockSpec(memory_space=pltpu.VMEM)
    dma = pltpu.SemaphoreType.DMA
    return pl.pallas_call(
        functools.partial(_body, p),
        in_specs=[any_, vm, any_, any_, vm, vm, vm, vm],
        out_specs=[any_, any_, any_],
        out_shape=[jax.ShapeDtypeStruct((t, d), BF), jax.ShapeDtypeStruct((3 * hc, d, dh), BF),
                   jax.ShapeDtypeStruct((5, 2, 2, R, d), BF)],
        scratch_shapes=[
            pltpu.VMEM((2, 2, 2 * nchip, 2, R, R), BF), pltpu.VMEM((2, 8, 2, R, R), BF), pltpu.VMEM((2, 6, 2, 2, R, R), BF),
            pltpu.VMEM((16, 2 * R, R), BF), pltpu.VMEM((16, 2 * R, R), BF),
            pltpu.VMEM((4, R, 2 * R), F32), pltpu.VMEM((4, R, 2 * R), F32), pltpu.VMEM((9, R, 2 * R), F32),
            pltpu.VMEM((9, 1, 2 * R), F32), pltpu.VMEM((9, 1, 2 * R), F32),
            dma((4,)), dma((3,)), dma((3, 4)), dma((5, 2, 3)), dma((5, 2, 2)), dma((2, 6)), dma((2, 6)), dma((16,)), dma((16,))],
        compiler_params=pltpu.CompilerParams(vmem_limit_bytes=VMEM_LIMIT, collective_id=0, has_side_effects=True),
        name="sublayer",
    )(x, g.reshape(1, d), wqkv, wo, *rot)[0]


def solution(mesh):
    p = mesh.shape["seq"]
    rows = P(("data", "seq"), None)

    def local(x, g, wqkv, wo):
        y = _sublayer(x, g, wqkv, wo, p)
        return y + jnp.minimum(lax.axis_index("seq"), 0).astype(BF)

    return jax.shard_map(local, mesh=mesh,
                         in_specs=(rows, P(None), P(None, None, None, None), P(None, None, None)),
                         out_specs=rows, check_vma=False)
```

```python
import functools

import jax
import jax.numpy as jnp
import numpy as np
from jax import lax
from jax.experimental import pallas as pl
from jax.experimental.pallas import tpu as pltpu
from jax.sharding import PartitionSpec as P

BF = jnp.bfloat16
F32 = jnp.float32
I32 = jnp.int32
VMEM_LIMIT = 63 * 2**20
R = 256

OWN, N1A, N1B, FWA, N2A, FWB, N2B = range(7)


TWO = range(2)


def _loop(n, body):
    return lax.fori_loop(0, n, body, 0)


def _odd(a):
    return lax.rem(a, 2)


def _half(a):
    return lax.div(a, 2)


def _rem3(a):
    return lax.rem(a, 3)


def _rem8(a):
    return lax.rem(a, 8)


def _div8(a):
    return lax.div(a, 8)


def _pick(i, values):
    out = jnp.asarray(values[0], I32)
    for n, v in enumerate(values[1:], 1):
        out = jnp.where(i == n, v, out)
    return out


def _body(p, x_ref, g_ref, w_ref, wo_ref, cosb, sinb, cosc, sinc, y_ref, wall, xb, kvs, qs, fb, ob, og,
          sa, sb, acc, ms, ls, ld_sem, wt_sem, wo_sem, xs_sem, xr_sem, fs_sem, fr_sem, os_sem, or_sem):
    nchip = p // 2
    ng = nchip // 2
    d = x_ref.shape[1]
    hl = 2
    hc = hl * ng
    hw = R // 2
    me = lax.axis_index("seq")
    chip, core = _half(me), _odd(me)
    grp = lax.rem(chip, ng)

    def ring(off):
        return lax.rem(chip + off + nchip, nchip)

    def send(src, dst, ssem, rsem, off, other):
        k = jnp.where(other, 1 - core, core) if not isinstance(other, int) else (1 - core if other else core)
        return pltpu.make_async_remote_copy(src, dst, ssem, rsem, device_id={"seq": 2 * ring(off) + k},
                                            device_id_type=pl.DeviceIdType.MESH)

    barrier = pltpu.get_barrier_semaphore()
    peers = [(0, 1)] + [(o, k) for o in (1, -1, 2, -2) for k in (0, 1)]
    for o, k in peers:
        pl.semaphore_signal(barrier, inc=1, device_id={"seq": 2 * ring(o) + (1 - core if k else core)},
                            device_id_type=pl.DeviceIdType.MESH)

    def x_send(slot, j, to, other):
        src = x_ref.at[pl.ds(0, R)] if (slot, j) == (2, 0) else xb.at[slot, j, 0]
        dst = xb.at[slot, j, 1] if other else xb.at[slot - to, j, 0]
        return send(src, dst, xs_sem.at[slot, j, 0 if other else (1 if to > 0 else 2)],
                    xr_sem.at[slot, j, 1] if other else xr_sem.at[slot - to, j, 0], to, other)

    def x_wait(slot, j, other):
        pltpu.make_async_copy(xb.at[slot, j, other], xb.at[slot, j, other], xr_sem.at[slot, j, other]).wait()

    nb = d // R

    def norm(ref):
        def rows32(i, c):
            rows = pl.ds(i * 32, 32)
            xf = ref[rows, :].astype(F32)
            y = xf * lax.rsqrt(jnp.mean(xf * xf, axis=-1, keepdims=True) + 1e-5) * g_ref[...]
            ref[rows, :] = y.astype(BF)
            return c
        _loop(R // 32, rows32)

    def start(xv, pin, pout):
        x1 = pltpu.make_async_copy(x_ref.at[pl.ds(R, R)], xv, ld_sem.at[0])
        x1.start()
        pl.semaphore_wait(barrier, len(peers))
        for to, other in ((1, 0), (-1, 0), (0, 1)):
            x_send(2, 0, to, other).start()
        x1.wait()
        norm(xv)
        out = pltpu.make_async_copy(xv, xb.at[2, 1, 0], ld_sem.at[1])
        out.start()
        out.wait()
        for to, other in ((1, 0), (-1, 0), (0, 1)):
            x_send(2, 1, to, other).start()

        def w_in(i):
            kind, b = _rem3(lax.div(i, nb) + 1), lax.rem(i, nb)
            return pltpu.make_async_copy(w_ref.at[pl.ds(b * R, R), kind, pl.ds(pl.multiple_of(core * hc, hc), hc)],
                                         pin.at[_odd(i)], wt_sem.at[_odd(i)])

        def kv_out(i):
            kind, b = lax.div(i, nb) + 1, lax.rem(i, nb)
            return pltpu.make_async_copy(pout.at[_odd(i)], wall.at[pl.ds(kind * hc, hc), pl.ds(b * R, R)],
                                         ld_sem.at[_odd(i)])

        def q_out(i):
            return pltpu.make_async_copy(pout.at[_odd(i), pl.ds(0, hl)],
                                         wall.at[pl.ds(hl * grp, hl), pl.ds(lax.rem(i, nb) * R, R)], ld_sem.at[_odd(i)])

        def put_kv(i):
            pout[_odd(i)] = jnp.swapaxes(pin[_odd(i)], 0, 1)

        def put_q(i):
            for gv in range(ng):
                @pl.when(grp == gv)
                def _(gv=gv):
                    pout[_odd(i), :hl] = jnp.swapaxes(pin[_odd(i), :, hl * gv:hl * gv + hl], 0, 1)

        def prep(put, out, lo, i, c):
            @pl.when(i + 1 < 3 * nb)
            def _():
                w_in(i + 1).start()
            w_in(i).wait()

            @pl.when(i >= lo + 2)
            def _():
                out(i - 2).wait()
            put(i)
            out(i).start()
            return c
        w_in(jnp.int32(0)).start()
        for put, out, lo, hi in ((put_kv, kv_out, 0, 2 * nb), (put_q, q_out, 2 * nb, 3 * nb)):
            lax.fori_loop(lo, hi, functools.partial(prep, put, out, lo), 0)
            for e in (2, 1):
                out(jnp.int32(hi - e)).wait()

    pl.run_scoped(start, pltpu.VMEM((R, d), BF), pltpu.VMEM((2, R, hc, R), BF), pltpu.VMEM((2, hc, R, R), BF))

    even = _odd(chip) == 0

    kb, qb = 4 * R, 2 * R
    EARLY, NEAR, HEAD0, FAR = range(4)

    def q_off(e):
        return jnp.where(e < 2, jnp.where(even, 2, -2), jnp.where(e < 4, -1, jnp.where(e < 6, 1, 0)))

    def o_send(i):
        e = _rem8(i)
        return send(ob.at[i], og.at[i], os_sem.at[i], or_sem.at[i], q_off(e), _odd(e) == 1)

    def around(reach):
        b = ring(-reach)
        wrapped = jnp.logical_or(chip < reach, chip + reach >= nchip)
        return jnp.where(wrapped, ring(reach + 1), 0), b

    def attend(ps, e):
        h = jnp.where(ps == HEAD0, 0, 1)
        i = 8 * h + e
        qc = ring(q_off(e))
        pb = 2 * qc + jnp.where(_odd(e) == 0, core, 1 - core)
        w1, b1 = around(1)
        w2, b2 = around(2)
        rest = jnp.logical_and(ps == NEAR, e >= 2)
        up2 = ring(2)
        low_ok, up_ok = b2 < qc, up2 < qc
        n0 = jnp.where(ps == FAR, w2, jnp.where(rest, b2, 0))
        n1 = jnp.where(ps == EARLY, b1, jnp.where(rest, up2, b2))
        w = jnp.where(ps == EARLY, w1, jnp.where(rest, jnp.where(low_ok, 1, 0), jnp.where(ps == NEAR, w2, nchip)))
        cnt = jnp.where(
            ps == EARLY, jnp.where(qc >= b1, w1 + qc - b1, qc),
            jnp.where(rest, jnp.where(low_ok, 1, 0) + jnp.where(up_ok, 1, 0),
                      jnp.where(ps == NEAR, jnp.where(qc >= b2, w2 + qc - b2, qc),
                                jnp.where(ps == HEAD0, qc, jnp.where(qc >= b2, b2 - w2, 0)))))
        last = jnp.logical_not(jnp.logical_or(rest, ps == FAR))
        sl = jnp.where(ps == HEAD0, 8, e)

        def keys_of(idx):
            return jnp.where(idx >= cnt, qc, jnp.where(idx < w, n0 + idx, n1 + idx - w))

        @pl.when(last)
        def _():
            acc[sl] = jnp.zeros((R, qb), F32)
            ms[sl] = jnp.full((1, qb), -jnp.inf, F32)
            ls[sl] = jnp.zeros((1, qb), F32)

        def scores(idx, dst):
            n = keys_of(idx)
            kblk = kvs[0, h, pl.ds(2 * n, 2)].reshape(kb, R)
            q = qs[h, e].reshape(qb, R)
            s = lax.dot_general(kblk, q, (((1,), (1,)), ((), ())), preferred_element_type=F32)
            dst[...] = s.reshape(dst.shape)

        def update(idx, src, masked, nk=4):
            n = keys_of(idx)
            s = src[:nk].reshape(nk * R, qb)
            if masked:
                kp = n * kb + lax.broadcasted_iota(I32, s.shape, 0)
                qp = pb * qb + lax.broadcasted_iota(I32, s.shape, 1)
                s = jnp.where(qp >= kp, s, -jnp.inf)
            mo = ms[sl]
            mn = jnp.maximum(mo, jnp.max(s, axis=0, keepdims=True))
            al = jnp.exp(mo - mn)
            pr = jnp.exp(s - mn)
            ls[sl] = ls[sl] * al + jnp.sum(pr, axis=0, keepdims=True)
            ms[sl] = mn
            vblk = kvs[1, h, pl.ds(2 * n, 2)]
            vblk = jnp.concatenate([vblk[a // 2, a % 2] for a in range(nk)], axis=-1)
            acc[sl] = acc[sl] * al + jnp.dot(vblk, pr.astype(BF), preferred_element_type=F32)

        @pl.when(jnp.logical_or(cnt > 0, last))
        def _():
            scores(0, sa)

            def two(u, c2):
                scores(2 * u + 1, sb)
                update(2 * u, sa, False)
                scores(2 * u + 2, sa)
                update(2 * u + 1, sb, False)
                return c2
            _loop(_half(cnt), two)
            odd = _odd(cnt) == 1

            @pl.when(jnp.logical_and(odd, last))
            def _():
                scores(cnt, sb)
                update(cnt - 1, sa, False)

            @pl.when(jnp.logical_and(odd, jnp.logical_not(last)))
            def _():
                update(cnt - 1, sa, False)

            for buf, par in ((sa, 0), (sb, 1)):
                for kk in TWO:
                    @pl.when(jnp.logical_and(last, jnp.logical_and(_odd(cnt) == par, _odd(pb) == kk)))
                    def _(buf=buf, kk=kk):
                        update(cnt, buf, True, 2 + 2 * kk)

        @pl.when(ps >= HEAD0)
        def _():
            out = (acc[sl] / ls[sl]).T.astype(BF)

            @pl.when(e == 6)
            def _():
                og[i] = out

            @pl.when(e != 6)
            def _():
                ob[i] = out

    def f_wait_head(hh):
        for j in TWO:
            for n in range(3):
                f_wait(j, 3 * hh + n)

    def attend_loop():
        busy = chip >= ng

        def send_head0(n):
            for k in range(n):
                o_send(jnp.int32(k)).start()

        def one(it, c):
            ps, e = 1 + _div8(it), _rem8(it)

            @pl.when(it == 8)
            def _():
                f_wait_head(0)

            @pl.when(it == 16)
            def _():
                f_wait_head(1)

            @pl.when(jnp.logical_and(it == 16, jnp.logical_not(busy)))
            def _():
                send_head0(6)
                o_send(jnp.int32(7)).start()
            attend(ps, e)

            @pl.when(jnp.logical_and(ps == FAR, e != 6))
            def _():
                o_send(8 + e).start()

            @pl.when(jnp.logical_and(busy, it == 14))
            def _():
                send_head0(6)

            @pl.when(jnp.logical_and(busy, it == 15))
            def _():
                o_send(e).start()
            return c
        _loop(24, one)

    def f_of(ph, st):
        f = _half(st)
        n = _rem3(f)
        return lax.div(f, 3), jnp.where(n == 1, jnp.where(ph == FWA, 0, 2), n), _pick(n, (1, 2, ng - 1))

    def is_fw(ph):
        return jnp.logical_or(ph == FWA, ph == FWB)

    def is_n2(ph):
        return jnp.logical_or(ph == N2A, ph == N2B)

    def head_of(ph, st):
        return _odd(st)

    def widx(ph, st):
        fh, _, fg = f_of(ph, st)
        near = _pick(_half(st), (hc, 2 * hc, 0)) + hl * grp + head_of(ph, st)
        fwd = hc * (1 + _odd(st)) + hl * lax.rem(grp + fg, ng) + fh
        return jnp.where(is_fw(ph), fwd, near)

    def w_load(wt, ph, st, gs):
        return pltpu.make_async_copy(wall.at[widx(ph, st)], wt.at[_rem3(gs)], wt_sem.at[_rem3(gs)])

    def steps_of(ph):
        return jnp.where(is_fw(ph), 12, 6)

    def next_step(ph, st):
        inside = st + 1 < steps_of(ph)
        return jnp.where(inside, ph, ph + 1), jnp.where(inside, st + 1, 0)

    def off_of(ph, m):
        a = jnp.where(ph == OWN, 0, jnp.where(ph <= N1B, 1, 2))
        return jnp.where(m < 2, -a, a)

    def chunk_of(ph, m):
        return jnp.where(ph == OWN, _half(m), jnp.where(jnp.logical_or(ph == N1B, ph >= FWB), 1, 0))

    def x_load(xv, ph, m):
        return pltpu.make_async_copy(xb.at[off_of(ph, m) + 2, chunk_of(ph, m), _odd(m)], xv.at[m], ld_sem.at[m])

    def block_of(ph, m):
        return 2 * ring(off_of(ph, m)) + jnp.where(_odd(m) == 0, core, 1 - core)

    def f_send(j, f):
        h, to = f // 3, (1, (2, -2)[j], -1)[f % 3]
        src_off = -2 if to > 0 else 2
        return send(fb.at[j, f], kvs.at[:, h, pl.ds(2 * ring(src_off), 2), j], fs_sem.at[j, f], fr_sem.at[j, f], to, 0)

    def f_wait(j, f):
        h, frm = f // 3, (-3, 4, 3)[f % 3]
        ref = kvs.at[:, h, pl.ds(2 * ring(frm), 2), j]
        pltpu.make_async_copy(ref, ref, fr_sem.at[j, f]).wait()

    def phase(xv, wt, cs, sn, res, ph, gs):
        def relay(j):
            for s in (1, 3):
                x_wait(s, j, 0)
                x_send(s, j, 1 if s == 1 else -1, 0).start()
                x_send(s, j, 0, 1).start()

        @pl.when(ph == OWN)
        def _():
            relay(0)

        @pl.when(ph == FWA)
        def _():
            def early(e, c):
                attend(jnp.int32(EARLY), e)
                return c
            lax.fori_loop(2, 8, early, 0)
        def share(j):
            for s in (0, 4):
                x_wait(s, j, 0)
                x_send(s, j, 0, 1).start()

        @pl.when(ph == FWA)
        def _():
            share(0)
        fw = is_fw(ph)
        raw = jnp.logical_or(ph == N1A, ph == FWA)

        def norms(lo, step=1):
            lax.fori_loop(0, 2, lambda m, c: (norm(xv.at[lo + step * m]), c)[1], 0)
        fresh = jnp.logical_not(is_n2(ph))

        @pl.when(fresh)
        def _():
            @pl.when(ph == OWN)
            def _():
                pltpu.make_async_copy(x_ref.at[pl.ds(0, R)], xv.at[0], ld_sem.at[0]).start()

            @pl.when(ph != OWN)
            def _():
                x_load(xv, ph, 0).start()
            x_load(xv, ph, 2).start()
            for m in range(4):
                b = block_of(ph, jnp.int32(m))
                rows = pl.ds(pl.multiple_of(chunk_of(ph, jnp.int32(m)) * R, R), R)
                cc, sc = cosc[pl.ds(b, 1), :], sinc[pl.ds(b, 1), :]
                cb, sb_ = cosb[rows, :], sinb[rows, :]
                cs[m] = cb * cc - sb_ * sc
                sn[m] = sb_ * cc + cb * sc
        @pl.when(raw)
        def _():
            for m in (0, 2):
                x_load(xv, ph, m).wait()
            norms(0, 2)
        for at, waits in ((OWN, ((2, 0), (2, 1))), (N1A, ((1, 0), (3, 0))), (N1B, ((1, 1), (3, 1))),
                          (FWA, ((0, 0), (4, 0))), (FWB, ((0, 1), (4, 1)))):
            @pl.when(ph == at)
            def _(waits=waits):
                for s, j in waits:
                    x_wait(s, j, 1)

        @pl.when(fresh)
        def _():
            for m in (1, 3):
                x_load(xv, ph, m).start()

        @pl.when(raw)
        def _():
            for m in (1, 3):
                x_load(xv, ph, m).wait()
            norms(1, 2)

        @pl.when(jnp.logical_and(fresh, jnp.logical_not(raw)))
        def _():
            for m in TWO:
                x_load(xv, ph, m).wait()

        @pl.when(ph == OWN)
        def _():
            norms(0)

        @pl.when(jnp.logical_or(ph == OWN, ph == N1B))
        def _():
            for m in (2, 3):
                x_load(xv, ph, m).wait()

        def step(st, gs):
            nph, nst = next_step(*next_step(ph, st))

            @pl.when(nph <= N2B)
            def _():
                w_load(wt, nph, nst, gs + 2).start()

            @pl.when(jnp.logical_and(ph == N1A, st == 4))
            def _():
                relay(1)

            @pl.when(jnp.logical_and(ph == N2A, st == 5))
            def _():
                share(1)

            @pl.when(jnp.logical_and(ph == FWB, st == 2))
            def _():
                for m in (2, 3):
                    x_load(xv, ph, m).wait()
            w_load(wt, ph, st, gs).wait()
            kind = jnp.where(fw, 1 + _odd(st), _pick(_half(st), (1, 2, 0)))
            fh, flo, _ = f_of(ph, st)
            n2q = jnp.logical_and(is_n2(ph), st >= 4)
            h = jnp.where(fw, fh, head_of(ph, st))
            lo = jnp.where(fw, flo, jnp.where(jnp.logical_and(n2q, even), 2, 0))
            cnt = jnp.where(jnp.logical_or(fw, n2q), 1, 2)
            f = _half(st)
            jf = jnp.where(ph == FWB, 1, 0)
            wslot = _rem3(gs)

            def dots(m):
                return [jnp.dot(xv[m + e], wt[wslot], preferred_element_type=F32) for e in TWO]

            @pl.when(kind != 2)
            def _():
                scale = jnp.where(kind == 0, R ** -0.5, 1.0).astype(F32)

                def two(u, c):
                    m = lo + 2 * u
                    av = dots(m)
                    for e in TWO:
                        a = av[e] * scale
                        a1, a2 = a[:, :hw], a[:, hw:]
                        cv, sv = cs[m + e], sn[m + e]
                        res[m + e] = jnp.concatenate([a1 * cv - a2 * sv, a2 * cv + a1 * sv], axis=-1).astype(BF)
                    return c
                _loop(cnt, two)

            @pl.when(kind == 2)
            def _():
                def two(u, c):
                    m = lo + 2 * u
                    av = dots(m)
                    for e in TWO:
                        res[m + e] = av[e].astype(BF).T
                    return c
                _loop(cnt, two)

            def put(m, c):
                blk = block_of(ph, m)
                j = chunk_of(ph, m)

                @pl.when(fw)
                def _():
                    fb[jf, f, kind - 1, _odd(blk)] = res[m]

                @pl.when(jnp.logical_and(jnp.logical_not(fw), kind > 0))
                def _():
                    kvs[kind - 1, h, blk, j] = res[m]

                @pl.when(kind == 0)
                def _():
                    o = off_of(ph, m)
                    qi = jnp.where(o == 0, 6, jnp.where(o == -1, 2, jnp.where(o == 1, 4, 0))) + _odd(m)
                    qs[h, qi, j] = res[m]
                return c
            lax.fori_loop(lo, lo + 2 * cnt, put, 0)

            for n in range(3):
                @pl.when(jnp.logical_and(ph == FWA, st == 2 * n + 1))
                def _(n=n):
                    f_send(0, n).start()

                @pl.when(jnp.logical_and(ph == FWB, st == 2 * n + 1))
                def _(n=n):
                    f_send(1, n).start()
                    if n == 0:
                        for m in (3, 4):
                            f_send(0, m).start()

                if n == 2:
                    @pl.when(jnp.logical_and(ph == FWA, st == 11))
                    def _():
                        f_send(0, 5).start()

                @pl.when(jnp.logical_and(ph == FWB, st == 2 * n + 7))
                def _(n=n):
                    f_send(1, n + 3).start()
            return gs + 1
        return lax.fori_loop(0, steps_of(ph), step, gs)

    def project(xv, wt, cs, sn, res):
        for n in TWO:
            w_load(wt, jnp.int32(OWN), jnp.int32(n), jnp.int32(n)).start()
        lax.fori_loop(0, N2B + 1, functools.partial(phase, xv, wt, cs, sn, res), jnp.int32(0))

    pl.run_scoped(project, pltpu.VMEM((4, R, d), BF), pltpu.VMEM((3, d, R), BF), pltpu.VMEM((4, R, hw), F32),
                  pltpu.VMEM((4, R, hw), F32), pltpu.VMEM((4, R, R), BF))

    attend_loop()

    dm = wo_ref.shape[2]
    nw = dm // 2
    cw = 2 * R
    ncol = nw // cw
    groups = ((0, 1, 2, 3), (4, 5, 6, 7), (8, 9, 14, 15), (10, 11, 12, 13))
    early = ((6, 7, 14, 15), groups[0], (4, 5, 8, 9), groups[3])

    def piece(n, k):
        return jnp.where(chip >= ng, _pick(n, [gr[k] for gr in groups]), _pick(n, [gr[k] for gr in early]))

    def wo_load(wv, n, half):
        sl, out = _rem3(2 * n + half), []
        for k in range(4):
            i = piece(n, k)
            gg = lax.rem(grp + _pick(_half(_rem8(i)), (2, 1, ng - 1, 0)), ng)
            head = hc * jnp.where(_odd(i) == 0, core, 1 - core) + hl * gg + _div8(i)
            out.append(pltpu.make_async_copy(wo_ref.at[head, :, pl.ds(half * nw, nw)], wv.at[sl, k], wo_sem.at[sl, k]))
        return out

    def wo_start(wv, n, half):
        @pl.when(n < len(groups))
        def _():
            for cp in wo_load(wv, n, half):
                cp.start()

    def finish(yb, wv):
        res = pltpu.make_async_copy(x_ref, yb, wt_sem.at[1])
        res.start()
        for half in TWO:
            wo_start(wv, jnp.int32(0), half)
        res.wait()
        tops = (sa, sb)

        for half in TWO:
            def fill(i, c, half=half):
                to = pl.ds(pl.multiple_of(half * nw + i * cw, cw), cw)
                tops[half][i] = yb[:R, to].astype(F32)
                acc[half * ncol + i] = yb[R:, to].astype(F32)
                return c
            _loop(ncol, fill)

        def out(n, c):
            for half in TWO:
                sl = _rem3(2 * n + half)
                wo_start(wv, n + 1, half)
                if half == 0:
                    for k in range(4):
                        i = piece(n, k)

                        @pl.when(_rem8(i) != 6)
                        def _(i=i):
                            o_send(i).wait()
                for cp in wo_load(wv, n, half):
                    cp.wait()
                oo = jnp.concatenate([og[piece(n, k)] for k in range(4)], axis=-1)

                def cols(i, c2, half=half, sl=sl, oo=oo):
                    at = pl.ds(pl.multiple_of(i * cw, cw), cw)
                    ww = jnp.concatenate([wv[sl, k, :, at] for k in range(4)], axis=0)
                    a = jnp.dot(oo, ww, preferred_element_type=F32)
                    tops[half][i] = tops[half][i] + a[:R]
                    acc[half * ncol + i] = acc[half * ncol + i] + a[R:]
                    return c2
                _loop(ncol, cols)

                @pl.when(n == len(groups) - 1)
                def _(half=half):
                    def store(i, c2):
                        to = pl.ds(pl.multiple_of(half * nw + i * cw, cw), cw)
                        yb[:R, to] = tops[half][i].astype(BF)
                        yb[R:, to] = acc[half * ncol + i].astype(BF)
                        pltpu.make_async_copy(yb.at[:, to], y_ref.at[:, to], wt_sem.at[0]).start()
                        return c2
                    _loop(ncol, store)
            return c
        _loop(len(groups), out)
        pltpu.make_async_copy(yb, y_ref, wt_sem.at[0]).wait()

    pl.run_scoped(finish, pltpu.VMEM((qb, dm), BF), pltpu.VMEM((3, 4, R, nw), BF))

    for j in TWO:
        for s in range(5):
            x_send(s, j, 0, 1).wait_send()
        for s, to in ((2, 1), (2, -1), (1, 1), (3, -1)):
            x_send(s, j, to, 0).wait_send()
        for f in range(6):
            f_send(j, f).wait_send()


def _sublayer(x, g, wqkv, wo, p):
    t, d = x.shape
    _, _, nh, dh = wqkv.shape
    hw = dh // 2
    nchip = p // 2
    hc = nh // 2
    inv = 10000.0 ** (-np.arange(hw) * 2.0 / dh)
    ab, ac = np.arange(t)[:, None] * inv, (np.arange(p) * t)[:, None] * inv
    rot = [jnp.asarray(f(a), F32) for a in (ab, ac) for f in (np.cos, np.sin)]
    any_ = pl.BlockSpec(memory_space=pl.ANY)
    vm = pl.BlockSpec(memory_space=pltpu.VMEM)
    dma = pltpu.SemaphoreType.DMA
    return pl.pallas_call(
        functools.partial(_body, p),
        in_specs=[any_, vm, any_, any_, vm, vm, vm, vm],
        out_specs=[any_, any_, any_],
        out_shape=[jax.ShapeDtypeStruct((t, d), BF), jax.ShapeDtypeStruct((3 * hc, d, dh), BF),
                   jax.ShapeDtypeStruct((5, 2, 2, R, d), BF)],
        scratch_shapes=[
            pltpu.VMEM((2, 2, 2 * nchip, 2, R, R), BF), pltpu.VMEM((2, 8, 2, R, R), BF), pltpu.VMEM((2, 6, 2, 2, R, R), BF),
            pltpu.VMEM((16, 2 * R, R), BF), pltpu.VMEM((16, 2 * R, R), BF),
            pltpu.VMEM((4, R, 2 * R), F32), pltpu.VMEM((4, R, 2 * R), F32), pltpu.VMEM((9, R, 2 * R), F32),
            pltpu.VMEM((9, 1, 2 * R), F32), pltpu.VMEM((9, 1, 2 * R), F32),
            dma((4,)), dma((3,)), dma((3, 4)), dma((5, 2, 3)), dma((5, 2, 2)), dma((2, 6)), dma((2, 6)), dma((16,)), dma((16,))],
        compiler_params=pltpu.CompilerParams(vmem_limit_bytes=VMEM_LIMIT, collective_id=0, has_side_effects=True),
        name="sublayer",
    )(x, g.reshape(1, d), wqkv, wo, *rot)[0]


def solution(mesh):
    p = mesh.shape["seq"]
    rows = P(("data", "seq"), None)

    def local(x, g, wqkv, wo):
        y = _sublayer(x, g, wqkv, wo, p)
        return y + jnp.minimum(lax.axis_index("seq"), 0).astype(BF)

    return jax.shard_map(local, mesh=mesh,
                         in_specs=(rows, P(None), P(None, None, None, None), P(None, None, None)),
                         out_specs=rows, check_vma=False)
```
